8 devices in a mesh: batch: 2 (over z, y), g: 4 (over x, core).
Axes of the slice: x: 2, y: 2, z: 1, core: 2. Of those that a mesh axis runs over, the one named last changes fastest.
Arguments:
- keys: float32 [65536], P(('batch', 'g')), parts along dimension 0
- payload: bfloat16 [65536, 768], P(('batch', 'g')), parts along dimension 0
Outputs:
- output 1: float32 [131072], P(('batch', 'g')), parts along dimension 0
- output 2: bfloat16 [131072, 768], P(('batch', 'g')), parts along dimension 0
- output 3: int32 [8], P(('batch', 'g')), parts along dimension 0
There are 2 independent parts. The reference program is written for one: setup_inputs(seed, part) draws one part's arguments, and reference() takes and returns one part's arrays. A program takes and returns all parts, laid end to end along the dimension named above; each array names one.
All inputs are finite; a program needn't handle non-finite values.
Results may differ from the reference program's by a relative error of at most 0.001.
Values are sent between devices in bfloat16 or wider.
A program may use at most 1 GiB of HBM per device.

```python
import math
import functools
import jax
import jax.numpy as jnp
from jax import lax

GROUP = 4
N_DEV = 8192
WIDTH = 768
SEGMENTS = 16
PART_ROWS = GROUP * N_DEV
OUT_ROWS = 2 * N_DEV
PAD_KEY = 128.0


def swap_into(perm_row, dev_id, target):
    cur_pos = jnp.argmax(perm_row == dev_id)
    displaced = perm_row[target]
    slot_ids = jnp.arange(perm_row.shape[0])
    return jnp.where(slot_ids == target, dev_id, jnp.where(slot_ids == cur_pos, displaced, perm_row))


def draw_keys(base):
    k_gap, k_exp, k_pick, k_block, k_heads, k_rest, k_local = jax.random.split(base, 7)
    seg_exp = jax.random.randint(k_exp, (SEGMENTS, 1), 0, 8)
    raw_bits = jax.random.randint(k_gap, (SEGMENTS, PART_ROWS // SEGMENTS), 0, 128)
    levels = jnp.cumsum((1 + jnp.right_shift(raw_bits, 7 - seg_exp)).reshape(-1))
    centered = levels - levels[PART_ROWS // 2]
    key_scale = 2.0 ** -(int(math.log2(PART_ROWS)) + 2)
    ranked_keys = centered.astype(jnp.float32) * key_scale
    picked = jax.random.permutation(k_pick, GROUP)
    hot_dev = picked[0]
    cold_dev = picked[1]
    hot_block = jax.random.randint(k_block, (), 0, GROUP - 1)
    block_ids = jnp.arange(GROUP)[:, None]
    head_owner = jax.vmap(functools.partial(jax.random.permutation, x=GROUP))(jax.random.split(k_heads, GROUP))
    hot_row = head_owner[hot_block]
    hot_pos = jnp.argmax(hot_row == hot_dev)
    hot_row = swap_into(hot_row, hot_dev, jnp.where(hot_pos >= GROUP // 2, hot_pos, GROUP - 1))
    head_owner = jnp.where(block_ids == hot_block, hot_row[None, :], head_owner)
    next_row = swap_into(head_owner[hot_block + 1], hot_dev, 0)
    head_owner = jnp.where(block_ids == hot_block + 1, next_row[None, :], head_owner)
    tail_owner = jnp.broadcast_to(jnp.repeat(jnp.arange(GROUP), N_DEV // GROUP - 1)[None, :], (GROUP, N_DEV - GROUP))
    tail_owner = jnp.where((block_ids == hot_block) & (tail_owner == cold_dev), hot_dev, tail_owner)
    tail_owner = jnp.where((block_ids == hot_block + 1) & (tail_owner == hot_dev), cold_dev, tail_owner)
    tail_owner = jax.vmap(jax.random.permutation)(jax.random.split(k_rest, GROUP), tail_owner)
    owners = jnp.concatenate([head_owner, tail_owner], axis=1).reshape(-1)
    rank_grid = jnp.argsort(owners, stable=True).reshape(GROUP, N_DEV)
    rank_grid = jax.vmap(jax.random.permutation)(jax.random.split(k_local, GROUP), rank_grid)
    return ranked_keys[rank_grid.reshape(-1)]


def setup_inputs(seed: int = 0, part: int = 0) -> dict:
    base = jax.random.fold_in(jax.random.key(seed), part)
    k_keys, k_rows = jax.random.split(base)
    keys = draw_keys(k_keys)
    payload = jax.random.normal(k_rows, (PART_ROWS, WIDTH), jnp.float32).astype(jnp.bfloat16)
    return {"keys": keys, "payload": payload}


def reference(keys, payload):
    local_sorted = jnp.sort(keys.reshape(GROUP, N_DEV), axis=1)
    samples = local_sorted[:, :: N_DEV // GROUP].reshape(-1)
    splitters = jnp.sort(samples)[GROUP + GROUP // 2 :: GROUP]
    sorted_all, sort_order = lax.sort((keys, jnp.arange(PART_ROWS, dtype=jnp.int32)), num_keys=1)
    edges = jnp.searchsorted(sorted_all, splitters, side="left").astype(jnp.int32)
    starts = jnp.concatenate([jnp.zeros((1,), jnp.int32), edges])
    stops = jnp.concatenate([edges, jnp.full((1,), PART_ROWS, jnp.int32)])
    counts = stops - starts
    slot_ids = jnp.arange(OUT_ROWS, dtype=jnp.int32)
    src_pos = jnp.minimum(starts[:, None] + slot_ids[None, :], PART_ROWS - 1)
    is_valid = slot_ids[None, :] < counts[:, None]
    out_keys = jnp.where(is_valid, sorted_all[src_pos], PAD_KEY)
    out_payload = jnp.where(is_valid[:, :, None], payload[sort_order[src_pos]], 0.0)
    return out_keys.reshape(-1), out_payload.reshape(-1, WIDTH), counts
```

```python
import functools
import jax
import jax.numpy as jnp
from jax import lax
from jax.experimental import pallas as pl
from jax.experimental.pallas import tpu as pltpu
from jax.sharding import PartitionSpec as P

PAD_KEY = 128.0
N = 8192
OUT = 2 * N
KR = N // 128
ZERO_ROW = 4 * N
UNITS = (1, 3, 2)
CAPS = (4128, 5152, 8192)
RB = 256
GRP = 64
CH = 1024
NS = 8
NO = 6
VMEM_LIMIT = 64 * 1024 * 1024 - 200 * 1024
MESH = pl.DeviceIdType.MESH
ANY = pl.BlockSpec(memory_space=pl.ANY)
SMEM = pl.BlockSpec(memory_space=pltpu.SMEM)
VMEM = pl.BlockSpec(memory_space=pltpu.VMEM)


def plan_kernel(key_ref, ord_ref, mkey_ref, code_ref, ordc_ref, meta_ref, keys8, ordr, ksend, krecv, osend, orecv):
    b = lax.axis_index("batch")
    g = lax.axis_index("g")
    core = lax.rem(g, 2)
    chip = g // 2
    sib = g + 1 - 2 * core
    me = b * 4 + g
    offs = [(db, dg) for db in (0, 1) for dg in range(4) if (db, dg) != (0, 0)]
    barrier = pltpu.get_barrier_semaphore()
    for db, dg in offs:
        pl.semaphore_signal(barrier, inc=1, device_id=(lax.rem(b + db, 2), lax.rem(g + dg, 4)), device_id_type=MESH)
    pl.semaphore_wait(barrier, len(offs))
    copies = []
    for k, (db, dg) in enumerate(offs):
        copies.append(
            pltpu.make_async_remote_copy(
                src_ref=key_ref,
                dst_ref=keys8.at[me],
                send_sem=ksend.at[k],
                recv_sem=krecv.at[k],
                device_id=(lax.rem(b + db, 2), lax.rem(g + dg, 4)),
                device_id_type=MESH,
            )
        )
    copies.append(
        pltpu.make_async_remote_copy(
            src_ref=ord_ref, dst_ref=ordr, send_sem=osend, recv_sem=orecv, device_id=(b, sib), device_id_type=MESH
        )
    )
    for c in copies:
        c.start()
    keys8[pl.ds(me, 1)] = key_ref[...].reshape(1, KR, 128)
    for c in copies:
        c.wait()

    def splitters(base):
        samples = []
        for s in range(4):
            for i in range(4):
                samples.append(jnp.broadcast_to(keys8[base + s, i * (KR // 4) : i * (KR // 4) + 1, :][:, 0:1], (1, 128)))
        ranks = []
        for k in range(16):
            r = jnp.zeros((1, 128), jnp.int32)
            for m in range(16):
                if m != k:
                    r = r + (samples[m] < samples[k]).astype(jnp.int32)
            ranks.append(r)
        out = []
        for j in (1, 2, 3):
            v = samples[0]
            for k in range(1, 16):
                v = jnp.where(ranks[k] == 4 * j + 2, samples[k], v)
            out.append(v)
        return out

    def below(slot, spl):
        return jnp.sum((keys8[slot] < spl).astype(jnp.int32))

    s1, s2, s3 = splitters(b * 4)
    _, o2, _ = splitters((1 - b) * 4)
    e = [below(b * 4 + s, s2) for s in range(4)]
    f = [below((1 - b) * 4 + s, o2) for s in range(4)]
    t_up, t_dn = 2 * N - e[0] - e[1], e[2] + e[3]
    h_up, h_dn = (t_up + 1) // 2, (t_dn + 1) // 2
    f_up, f_dn = 2 * N - f[0] - f[1], f[2] + f[3]
    worst = jnp.maximum(jnp.maximum(h_up, h_dn), jnp.maximum((f_up + 1) // 2, (f_dn + 1) // 2))
    first = chip == 0
    m0 = jnp.where(first, N - e[0], e[2])
    base0 = jnp.where(first, e[0], 0)
    base1 = jnp.where(first, e[1], 0)
    total = jnp.where(first, t_up, t_dn)
    half = jnp.where(first, h_up, h_dn)
    meta_ref[0] = core * half
    meta_ref[1] = jnp.where(core == 0, half, total)
    meta_ref[2] = m0
    meta_ref[3] = base0
    meta_ref[4] = N + base1 - m0
    meta_ref[6] = sum((worst > c).astype(jnp.int32) for c in CAPS[:-1])
    om0 = jnp.where(first, e[2], N - e[0])
    ob0 = jnp.where(first, 0, e[0])
    ob1 = jnp.where(first, 0, e[1])
    ohalf = jnp.where(first, h_dn, h_up)
    own_ord = ord_ref[...].astype(jnp.int32)
    sib_ord = ordr[...].astype(jnp.int32) + N
    ordc_ref[pl.ds(core, 1)] = own_ord.reshape(1, KR, 128)
    ordc_ref[pl.ds(1 - core, 1)] = sib_ord.reshape(1, KR, 128)
    big = jnp.full((1, 128), PAD_KEY, jnp.float32)
    lo = jnp.where(g == 0, -big, jnp.where(g == 1, s1, jnp.where(g == 2, s2, s3)))
    hi = jnp.where(g == 0, s1, jnp.where(g == 1, s2, jnp.where(g == 2, s3, big)))
    pos = lax.broadcasted_iota(jnp.int32, (KR, 128), 0) * 128 + lax.broadcasted_iota(jnp.int32, (KR, 128), 1)

    def crossed(p):
        second = p >= ohalf
        q = jnp.where(second, p - ohalf, p)
        return 2 * N + q + jnp.where(second == (core == 1), 0, N)

    other = b * 4 + (1 - chip) * 2
    count = jnp.zeros((), jnp.int32)
    entries = (
        (b * 4 + g, own_ord),
        (b * 4 + sib, sib_ord),
        (other, crossed(pos - ob0)),
        (other + 1, crossed(pos - ob1 + om0)),
    )
    for n, (slot, code) in enumerate(entries):
        k = keys8[slot]
        mine = (k >= lo) & (k < hi)
        mkey_ref[n] = jnp.where(mine, k, PAD_KEY)
        code_ref[n] = jnp.where(mine, code, ZERO_ROW)
        count = count + jnp.sum(mine.astype(jnp.int32))
    meta_ref[5] = count


def plan(skeys, sord):
    return pl.pallas_call(
        plan_kernel,
        out_shape=(
            jax.ShapeDtypeStruct((4, KR, 128), jnp.float32),
            jax.ShapeDtypeStruct((4, KR, 128), jnp.int32),
            jax.ShapeDtypeStruct((2, KR, 128), jnp.int32),
            jax.ShapeDtypeStruct((8,), jnp.int32),
        ),
        in_specs=[VMEM, VMEM],
        out_specs=(VMEM, VMEM, VMEM, SMEM),
        scratch_shapes=[
            pltpu.VMEM((8, KR, 128), jnp.float32),
            pltpu.VMEM((KR, 128), jnp.float32),
            pltpu.SemaphoreType.DMA((7,)),
            pltpu.SemaphoreType.DMA((7,)),
            pltpu.SemaphoreType.DMA,
            pltpu.SemaphoreType.DMA,
        ],
        name="plan",
        compiler_params=pltpu.CompilerParams(collective_id=0, has_side_effects=True),
    )(skeys, sord)


def load_rows(units, parts, src, stage, lsem):
    chunks = [(r, c, k, base + c, min(CH, rows - c)) for r, rows, k, base in parts for c in range(0, rows, CH)]

    def cp(n):
        r, c, k, _, m = chunks[n]
        s = n % NS
        return pltpu.make_async_copy(
            r.at[pl.ds(c, m), pl.ds(k * 128, units * 128)], stage.at[s, pl.ds(0, m)], lsem.at[s]
        )

    for n in range(min(NS, len(chunks))):
        cp(n).start()
    for n, (_, _, _, at, m) in enumerate(chunks):
        cp(n).wait()
        s = n % NS

        def widen(i, carry):
            for q in (0, 16):
                x = stage[s, pl.ds(i * 32 + q, 16), :].astype(jnp.float32)
                for u in range(units):
                    src[u, pl.ds(at + i * 32 + q, 16), :] = x[:, u * 128 : (u + 1) * 128]
            return carry

        lax.fori_loop(0, m // 32, widen, 0)
        if n + NS < len(chunks):
            cp(n + NS).start()


def emit(units, tmp, ost, slot, rows):
    for r in range(0, rows, 16):
        for u in range(units):
            ost[slot, r : r + 16, u * 128 : (u + 1) * 128] = tmp[u, r : r + 16, :].astype(jnp.bfloat16)


def pack_kernel(units, k0, ord_ref, meta_ref, own, sibl, out, src, stage, tmp, ost, lsem, osem):
    load_rows(units, [(own, N, k0, 0), (sibl, N, k0, N)], src, stage, lsem)
    p0, pend, m0, off0, off1 = (meta_ref[i] for i in range(5))
    cap = out.shape[0]
    pb = ost.shape[1]
    nb = (pend - p0 + pb - 1) // pb

    def ocp(i, slot):
        return pltpu.make_async_copy(ost.at[slot], out.at[pl.ds(pl.multiple_of(i * pb, pb), pb)], osem.at[slot])

    def block(i, carry):
        slot = lax.rem(i, NO)

        @pl.when(i >= NO)
        def _():
            ocp(i - NO, slot).wait()

        def group(q, c2):
            start = p0 + i * pb + q * 32
            whole = (start + 32 <= pend) & ((start + 32 <= m0) | (start >= m0))

            @pl.when(whole)
            def _():
                at = start + jnp.where(start >= m0, off1, off0)
                for j in range(32):
                    r = ord_ref[at + j]
                    for u in range(units):
                        tmp[u, pl.ds(q * 32 + j, 1), :] = src[u, pl.ds(r, 1), :]

            @pl.when(jnp.logical_not(whole))
            def _():
                def one(j, c3):
                    p = start + j
                    at = p + jnp.where(p >= m0, off1, off0)
                    r = ord_ref[jnp.minimum(at, 2 * N - 1)]
                    for u in range(units):
                        tmp[u, pl.ds(q * 32 + j, 1), :] = src[u, pl.ds(r, 1), :]
                    return c3

                lax.fori_loop(0, 32, one, 0)

            return c2

        lax.fori_loop(0, pb // 32, group, 0)
        emit(units, tmp, ost, slot, pb)
        ocp(i, slot).start()
        return carry

    lax.fori_loop(0, nb, block, 0)
    for t in range(NO):

        @pl.when(nb > t)
        def _():
            ocp(nb - 1 - t, lax.rem(nb - 1 - t, NO)).wait()


def pack_block(cap):
    return max(b for b in range(32, RB + 1, 32) if cap % b == 0)


def pack(units, k0, cap, order, meta, own, sibl):
    pb = pack_block(cap)
    return pl.pallas_call(
        functools.partial(pack_kernel, units, k0),
        out_shape=jax.ShapeDtypeStruct((cap, units * 128), jnp.bfloat16),
        in_specs=[SMEM, SMEM, ANY, ANY],
        out_specs=ANY,
        scratch_shapes=[
            pltpu.VMEM((units, 2 * N, 128), jnp.float32),
            pltpu.VMEM((NS, CH, units * 128), jnp.bfloat16),
            pltpu.VMEM((units, pb, 128), jnp.float32),
            pltpu.VMEM((NO, pb, units * 128), jnp.bfloat16),
            pltpu.SemaphoreType.DMA((NS,)),
            pltpu.SemaphoreType.DMA((NO,)),
        ],
        name=f"pack{k0}",
        cost_estimate=pl.CostEstimate(flops=0, transcendentals=0, bytes_accessed=2 * N * units * 256 + 8_000_000),
        compiler_params=pltpu.CompilerParams(vmem_limit_bytes=VMEM_LIMIT),
    )(order, meta, own, sibl)


def zero_kernel(meta_ref, out, zeros, sem):
    zeros[...] = jnp.zeros_like(zeros)
    nb = (meta_ref[5] + RB - 1) // RB

    def cp(i):
        return pltpu.make_async_copy(zeros, out.at[pl.ds(pl.multiple_of(i * RB, RB), RB)], sem)

    def go(i, c):
        cp(i).start()
        return c

    def end(i, c):
        cp(i).wait()
        return c

    lax.fori_loop(nb, OUT // RB, go, 0)
    lax.fori_loop(nb, OUT // RB, end, 0)


def zero_tail(meta, width):
    return pl.pallas_call(
        zero_kernel,
        out_shape=jax.ShapeDtypeStruct((OUT, width), jnp.bfloat16),
        in_specs=[SMEM],
        out_specs=ANY,
        scratch_shapes=[pltpu.VMEM((RB, width), jnp.bfloat16), pltpu.SemaphoreType.DMA],
        name="zero",
        cost_estimate=pl.CostEstimate(flops=0, transcendentals=0, bytes_accessed=OUT * width),
        compiler_params=pltpu.CompilerParams(vmem_limit_bytes=8 * 1024 * 1024),
    )(meta)


def final_kernel(units, k0, cap, idx_ref, meta_ref, own, sibl, rown, rsib, prev, out, src, stage, tmp, ost, lsem, osem):
    src[:, ZERO_ROW : ZERO_ROW + 8, :] = jnp.zeros((units, 8, 128), jnp.float32)
    parts = [(own, N, k0, 0), (sibl, N, k0, N), (rown, cap, 0, 2 * N), (rsib, cap, 0, 3 * N)]
    load_rows(units, parts, src, stage, lsem)
    nb = (meta_ref[5] + RB - 1) // RB

    def ocp(i, slot):
        return pltpu.make_async_copy(
            ost.at[slot], out.at[pl.ds(pl.multiple_of(i * RB, RB), RB), pl.ds(k0 * 128, units * 128)], osem.at[slot]
        )

    def block(i, carry):
        slot = lax.rem(i, NO)

        @pl.when(i >= NO)
        def _():
            ocp(i - NO, slot).wait()

        def group(q, c2):
            for j in range(GRP):
                r = idx_ref[i * RB + q * GRP + j]
                for u in range(units):
                    tmp[u, pl.ds(q * GRP + j, 1), :] = src[u, pl.ds(r, 1), :]
            return c2

        lax.fori_loop(0, RB // GRP, group, 0)
        emit(units, tmp, ost, slot, RB)
        ocp(i, slot).start()
        return carry

    lax.fori_loop(0, nb, block, 0)
    for t in range(NO):

        @pl.when(nb > t)
        def _():
            ocp(nb - 1 - t, lax.rem(nb - 1 - t, NO)).wait()


def final(units, k0, cap, idx, meta, own, sibl, rown, rsib, prev):
    return pl.pallas_call(
        functools.partial(final_kernel, units, k0, cap),
        out_shape=jax.ShapeDtypeStruct(prev.shape, prev.dtype),
        in_specs=[SMEM, SMEM, ANY, ANY, ANY, ANY, ANY],
        out_specs=ANY,
        input_output_aliases={6: 0},
        scratch_shapes=[
            pltpu.VMEM((units, ZERO_ROW + 8, 128), jnp.float32),
            pltpu.VMEM((NS, CH, units * 128), jnp.bfloat16),
            pltpu.VMEM((units, RB, 128), jnp.float32),
            pltpu.VMEM((NO, RB, units * 128), jnp.bfloat16),
            pltpu.SemaphoreType.DMA((NS,)),
            pltpu.SemaphoreType.DMA((NO,)),
        ],
        name=f"final{k0}",
        cost_estimate=pl.CostEstimate(flops=0, transcendentals=0, bytes_accessed=4 * N * units * 256 + 10_000_000),
        compiler_params=pltpu.CompilerParams(vmem_limit_bytes=VMEM_LIMIT),
    )(idx, meta, own, sibl, rown, rsib, prev)


SIBLING = [(0, 1), (1, 0), (2, 3), (3, 2)]
ACROSS = [(0, 2), (2, 0), (1, 3), (3, 1)]


def deliver(cap, order, meta, mkeys, codes, own, sibl):
    width = own.shape[1]
    starts = [sum(UNITS[:i]) for i in range(len(UNITS))]
    packed = []
    for i, (u, k0) in enumerate(zip(UNITS, starts)):
        if i:
            meta, _ = lax.optimization_barrier((meta, packed[-1]))
        packed.append(pack(u, k0, cap, order, meta, own, sibl))
        if i == 0:
            mkeys, codes, meta_out, _ = lax.optimization_barrier((mkeys, codes, meta, packed[0]))
    out = zero_tail(meta_out, width)
    out_keys, idx = lax.sort((mkeys.reshape(-1), codes.reshape(-1)), num_keys=1)
    out_keys, idx = out_keys[:OUT], idx[:OUT]
    for u, k0, p in zip(UNITS, starts, packed):
        got = lax.ppermute(p, "g", ACROSS)
        relayed = lax.ppermute(got, "g", SIBLING)
        out = final(u, k0, cap, idx, meta, own, sibl, got, relayed, out)
    return out_keys, out


def solution(mesh):
    def local_part(keys_loc, rows_loc):
        sibl = lax.ppermute(rows_loc, "g", SIBLING)
        skeys, sord = lax.sort((keys_loc, lax.iota(jnp.int32, N)), num_keys=1)
        mkeys, codes, ordc, meta = plan(skeys.reshape(KR, 128), sord.astype(jnp.float32).reshape(KR, 128))
        out_keys, out_rows = lax.switch(
            meta[6],
            [functools.partial(deliver, c) for c in CAPS],
            ordc.reshape(-1),
            meta,
            mkeys,
            codes,
            rows_loc,
            sibl,
        )
        return out_keys, out_rows, meta[5:6]

    row_spec = P(("batch", "g"))
    mat_spec = P(("batch", "g"), None)
    return jax.shard_map(
        local_part, mesh=mesh, in_specs=(row_spec, mat_spec), out_specs=(row_spec, mat_spec, row_spec), check_vma=False
    )
```

```python
import functools
import jax
import jax.numpy as jnp
from jax import lax
from jax.experimental import pallas as pl
from jax.experimental.pallas import tpu as pltpu
from jax.sharding import PartitionSpec as P


PAD_KEY = 128.0
N = 8192
OUT = 2 * N
KR = N // 128
ZERO_ROW = 4 * N
UNITS = (1, 2, 2, 1)
CAPS = (4128, 5152, 8192)
RB = 256
FB = 512
GRP = 64
CH = 1024
NS = 8
NO = 6
FO = 4
VMEM_LIMIT = 64 * 1024 * 1024 - 200 * 1024
MESH = pl.DeviceIdType.MESH
ANY = pl.BlockSpec(memory_space=pl.ANY)
SMEM = pl.BlockSpec(memory_space=pltpu.SMEM)
VMEM = pl.BlockSpec(memory_space=pltpu.VMEM)


def logical_bit(shape, b):
    if b < 3:
        return lax.broadcasted_iota(jnp.int32, shape, 1) >> b & 1
    if b < 6:
        return lax.broadcasted_iota(jnp.int32, shape, 0) >> (b - 3) & 1
    lane = lax.broadcasted_iota(jnp.int32, shape, 2)
    return lane >> 6 & 1 if b == 6 else lane >> (b - 7) & 1


def sort_keys(key):
    shape = (8, 8, 128)
    key = key.reshape(shape)
    rows = lax.broadcasted_iota(jnp.int32, (KR, 128), 0)
    place = (rows * 128 + lax.broadcasted_iota(jnp.int32, (KR, 128), 1)).astype(jnp.float32).reshape(shape)

    def partner(x, b, low):
        if 3 <= b < 6:
            d = 1 << (b - 3)
            return jnp.concatenate([x[v ^ d][None] for v in range(8)], 0)
        axis, d, size = (1, 1 << b, 8) if b < 3 else (2, 64 if b == 6 else 1 << (b - 7), 128)
        if 2 * d == size:
            return pltpu.roll(x, d, axis)
        return jnp.where(low, pltpu.roll(x, size - d, axis), pltpu.roll(x, d, axis))

    for k in range(1, 14):
        for b in range(k - 1, -1, -1):
            low = logical_bit(shape, b) == 0
            want_min = low if k == 13 else low == (logical_bit(shape, k) == 0)
            pk, pp = partner(key, b, low), partner(place, b, low)
            take = (pk < key) == want_min
            key, place = jnp.where(take, pk, key), jnp.where(take, pp, place)

    def flat(x):
        t = jnp.transpose(x.reshape(KR, 128))
        return jnp.concatenate([t[:64], t[64:]], axis=1)

    return flat(key), flat(place)


def plan_kernel(
    raw_ref, own, gkey_ref, code_ref, ordc_ref, meta_ref, sib0, key_ref, ord_ref, keys8, ordr, ksend, krecv, osend, orecv,
    rsend, rrecv
):
    b = lax.axis_index("batch")
    g = lax.axis_index("g")
    core = lax.rem(g, 2)
    chip = g // 2
    sib = g + 1 - 2 * core
    me = b * 4 + g
    offs = [(db, dg) for db in (0, 1) for dg in range(4) if (db, dg) != (0, 0)]
    sorted_keys, places = sort_keys(raw_ref[...] * jnp.where(core == 1, -1.0, 1.0))
    key_ref[...] = sorted_keys
    ord_ref[...] = places
    keys8[pl.ds(me, 1)] = sorted_keys.reshape(1, KR, 128)
    barrier = pltpu.get_barrier_semaphore()
    for db, dg in offs:
        pl.semaphore_signal(barrier, inc=1, device_id=(lax.rem(b + db, 2), lax.rem(g + dg, 4)), device_id_type=MESH)
    pl.semaphore_wait(barrier, len(offs))
    copies = []
    for k, (db, dg) in enumerate(offs):
        copies.append(
            pltpu.make_async_remote_copy(
                src_ref=key_ref,
                dst_ref=keys8.at[me],
                send_sem=ksend.at[k],
                recv_sem=krecv.at[k],
                device_id=(lax.rem(b + db, 2), lax.rem(g + dg, 4)),
                device_id_type=MESH,
            )
        )
    copies.append(
        pltpu.make_async_remote_copy(
            src_ref=ord_ref, dst_ref=ordr, send_sem=osend, recv_sem=orecv, device_id=(b, sib), device_id_type=MESH
        )
    )
    for c in copies:
        c.start()
    slab = pltpu.make_async_remote_copy(
        src_ref=own.at[:, pl.ds(0, sib0.shape[1])],
        dst_ref=sib0,
        send_sem=rsend,
        recv_sem=rrecv,
        device_id=(b, sib),
        device_id_type=MESH,
    )
    slab.start()
    for c in copies:
        c.wait()

    def keys_of(base, s):
        k = keys8[base + s]
        return k * -1.0 if s % 2 else k

    def splitters(base):
        samples = []
        for s in range(4):
            for i in range(4):
                r = i * (KR // 4)
                if s % 2:
                    v = keys8[base + s, KR - 1 - r : KR - r, :][:, 127:128] * -1.0
                else:
                    v = keys8[base + s, r : r + 1, :][:, 0:1]
                samples.append(jnp.broadcast_to(v, (1, 128)))
        ranks = []
        for k in range(16):
            r = jnp.zeros((1, 128), jnp.int32)
            for m in range(16):
                if m != k:
                    r = r + (samples[m] < samples[k]).astype(jnp.int32)
            ranks.append(r)
        out = []
        for j in (1, 2, 3):
            v = samples[0]
            for k in range(1, 16):
                v = jnp.where(ranks[k] == 4 * j + 2, samples[k], v)
            out.append(v)
        return out

    def below(base, s, spl):
        return jnp.sum((keys_of(base, s) < spl).astype(jnp.int32))

    s1, s2, s3 = splitters(b * 4)
    _, o2, _ = splitters((1 - b) * 4)
    e = [below(b * 4, s, s2) for s in range(4)]
    f = [below((1 - b) * 4, s, o2) for s in range(4)]
    t_up, t_dn = 2 * N - e[0] - e[1], e[2] + e[3]
    h_up, h_dn = (t_up + 1) // 2, (t_dn + 1) // 2
    f_up, f_dn = 2 * N - f[0] - f[1], f[2] + f[3]
    worst = jnp.maximum(jnp.maximum(h_up, h_dn), jnp.maximum((f_up + 1) // 2, (f_dn + 1) // 2))
    first = chip == 0
    m0 = jnp.where(first, N - e[0], e[2])
    base0 = jnp.where(first, e[0], 0)
    base1 = jnp.where(first, 0, N - e[3])
    total = jnp.where(first, t_up, t_dn)
    half = jnp.where(first, h_up, h_dn)
    meta_ref[0] = core * half
    meta_ref[1] = jnp.where(core == 0, half, total)
    meta_ref[2] = m0
    meta_ref[3] = base0
    meta_ref[4] = N + base1 - m0
    meta_ref[6] = sum((worst > c).astype(jnp.int32) for c in CAPS[:-1])
    own_ord = ord_ref[...].astype(jnp.int32)
    sib_ord = ordr[...].astype(jnp.int32) + N
    orders = [jnp.where(core == c, own_ord, sib_ord) for c in (0, 1)]
    for c in (0, 1):
        ordc_ref[c] = orders[c]
    big = jnp.full((1, 128), PAD_KEY, jnp.float32)
    lo = jnp.where(g == 0, -big, jnp.where(g == 1, s1, jnp.where(g == 2, s2, s3)))
    hi = jnp.where(g == 0, s1, jnp.where(g == 1, s2, jnp.where(g == 2, s3, big)))
    pos = lax.broadcasted_iota(jnp.int32, (KR, 128), 0) * 128 + lax.broadcasted_iota(jnp.int32, (KR, 128), 1)
    shifts = (-e[0], N - e[0], 0, e[2] + e[3] - N)
    n_lo = jnp.zeros((KR, 128), jnp.int32)
    n_hi = jnp.zeros((KR, 128), jnp.int32)
    for s in range(4):
        k = keys_of(b * 4, s)
        n_lo = n_lo + (k < lo).astype(jnp.int32)
        n_hi = n_hi + (k < hi).astype(jnp.int32)
        p = pos + shifts[s]
        split = h_up if s < 2 else h_dn
        second = p >= split
        q = jnp.where(second, p - split, p)
        crossed = 2 * N + q + jnp.where(second == (core == 1), 0, N)
        gkey_ref[s] = k
        code_ref[s] = jnp.where(chip == s // 2, orders[s % 2], crossed)
    before = jnp.sum(n_lo)
    meta_ref[5] = jnp.sum(n_hi) - before
    meta_ref[7] = before
    slab.wait()


def plan(keys, rows):
    return pl.pallas_call(
        plan_kernel,
        out_shape=(
            jax.ShapeDtypeStruct((4, KR, 128), jnp.float32),
            jax.ShapeDtypeStruct((4, KR, 128), jnp.int32),
            jax.ShapeDtypeStruct((2, KR, 128), jnp.int32),
            jax.ShapeDtypeStruct((8,), jnp.int32),
            jax.ShapeDtypeStruct((N, UNITS[0] * 128), jnp.bfloat16),
        ),
        in_specs=[VMEM, ANY],
        out_specs=(VMEM, VMEM, VMEM, SMEM, ANY),
        scratch_shapes=[
            pltpu.VMEM((KR, 128), jnp.float32),
            pltpu.VMEM((KR, 128), jnp.float32),
            pltpu.VMEM((8, KR, 128), jnp.float32),
            pltpu.VMEM((KR, 128), jnp.float32),
            pltpu.SemaphoreType.DMA((7,)),
            pltpu.SemaphoreType.DMA((7,)),
            pltpu.SemaphoreType.DMA,
            pltpu.SemaphoreType.DMA,
            pltpu.SemaphoreType.DMA,
            pltpu.SemaphoreType.DMA,
        ],
        name="plan",
        compiler_params=pltpu.CompilerParams(collective_id=0, has_side_effects=True),
    )(keys, rows)


def exchange(key, code, bit, down_bit):
    rows = key.shape[0]
    if bit >= 10:
        d = 1 << (bit - 7)
        keys, codes = [], []
        for r in range(0, rows, 2 * d):
            a, c = key[r : r + d], key[r + d : r + 2 * d]
            x, y = code[r : r + d], code[r + d : r + 2 * d]
            down = down_bit is not None and (r * 128) >> down_bit & 1
            swap = a < c if down else c < a
            keys += [jnp.where(swap, c, a), jnp.where(swap, a, c)]
            codes += [jnp.where(swap, y, x), jnp.where(swap, x, y)]
        return jnp.concatenate(keys, 0), jnp.concatenate(codes, 0)
    if bit >= 7:
        axis, d, size = 1, 1 << (bit - 7), 8
    else:
        axis, d, size = 2, 1 << bit, 128
    shape = (rows // 8, 8, 128)
    k3, c3 = key.reshape(shape), code.reshape(shape)
    low = lax.broadcasted_iota(jnp.int32, shape, axis) & d == 0
    want_min = low
    if down_bit is not None:
        up = lax.broadcasted_iota(jnp.int32, shape, 0) >> (down_bit - 10) & 1 == 0
        want_min = low == up

    def partner(x):
        return jnp.where(low, pltpu.roll(x, size - d, axis), pltpu.roll(x, d, axis))

    pk, pc = partner(k3), partner(c3)
    take = (pk < k3) == want_min
    return jnp.where(take, pk, k3).reshape(key.shape), jnp.where(take, pc, c3).reshape(key.shape)


def merge_kernel(key_ref, code_ref, okey_ref, ocode_ref):
    key, code = key_ref[...], code_ref[...]
    for bit in range(13, -1, -1):
        key, code = exchange(key, code, bit, 14)
    for bit in range(14, -1, -1):
        key, code = exchange(key, code, bit, None)
    okey_ref[...] = key
    ocode_ref[...] = code


def merge(keys, codes):
    shape = (4 * KR, 128)
    return pl.pallas_call(
        merge_kernel,
        out_shape=(jax.ShapeDtypeStruct(shape, jnp.float32), jax.ShapeDtypeStruct(shape, jnp.int32)),
        in_specs=[VMEM, VMEM],
        out_specs=(VMEM, VMEM),
        name="merge",
        cost_estimate=pl.CostEstimate(flops=0, transcendentals=0, bytes_accessed=10_000_000),
        compiler_params=pltpu.CompilerParams(vmem_limit_bytes=16 * 1024 * 1024),
    )(keys.reshape(shape), codes.reshape(shape))


def load_rows(units, parts, src, stage, lsem):
    chunks = [(r, c, k, base + c, min(CH, rows - c)) for r, rows, k, base in parts for c in range(0, rows, CH)]

    def cp(n):
        r, c, k, _, m = chunks[n]
        s = n % NS
        return pltpu.make_async_copy(
            r.at[pl.ds(c, m), pl.ds(k * 128, units * 128)], stage.at[s, pl.ds(0, m)], lsem.at[s]
        )

    for n in range(min(NS, len(chunks))):
        cp(n).start()
    for n, (_, _, _, at, m) in enumerate(chunks):
        cp(n).wait()
        s = n % NS
        step = 128 if m % 128 == 0 else 32

        def widen(i, carry):
            for q in range(0, step, 16):
                x = stage[s, pl.ds(i * step + q, 16), :].astype(jnp.float32)
                for u in range(units):
                    src[u, pl.ds(at + i * step + q, 16), :] = x[:, u * 128 : (u + 1) * 128]
            return carry

        lax.fori_loop(0, m // step, widen, 0)
        if n + NS < len(chunks):
            cp(n + NS).start()


def first_unit(ref, units, k0):
    return 0 if ref.shape[1] == units * 128 else k0


def narrow(units, tmp, ost, slot, row):
    for r in range(0, GRP, 16):
        for u in range(units):
            ost[slot, row + r : row + r + 16, u * 128 : (u + 1) * 128] = tmp[u, r : r + 16, :].astype(jnp.bfloat16)


def gather_block(units, rows, index, src, tmps, ost, slot):
    for q in range(rows // GRP):
        tmp = tmps[q % 2]
        for j in range(GRP):
            r = index(q * GRP + j)
            for u in range(units):
                tmp[u, j : j + 1, :] = src[u, pl.ds(r, 1), :]
        if q:
            narrow(units, tmps[(q - 1) % 2], ost, slot, (q - 1) * GRP)
    narrow(units, tmps[(rows // GRP - 1) % 2], ost, slot, rows - GRP)


def pack_kernel(
    units, k0, order, meta_ref, own, sibl, out, src, stage, tmp_a, tmp_b, ost, ord_ref, lsem, osem, tsem, isem
):
    listed = pltpu.make_async_copy(order, ord_ref, isem)
    listed.start()
    load_rows(units, [(own, N, k0, 0), (sibl, N, first_unit(sibl, units, k0), N)], src, stage, lsem)
    listed.wait()
    p0, pend, m0, off0, off1 = (meta_ref[i] for i in range(5))
    full, rest = divmod(out.shape[0], RB)
    nb = jnp.minimum((pend - p0 + RB - 1) // RB, full)

    def ocp(i, slot):
        return pltpu.make_async_copy(ost.at[slot], out.at[pl.ds(pl.multiple_of(i * RB, RB), RB)], osem.at[slot])

    def mixed(start, slot, rows):
        def some(i, carry):
            for j in range(16):
                p = start + i * 16 + j
                at = p + jnp.where(p >= m0, off1, off0)
                r = ord_ref[jnp.minimum(at, 2 * N - 1)]
                for u in range(units):
                    tmp_a[u, j : j + 1, :] = src[u, pl.ds(r, 1), :]
            for u in range(units):
                ost[slot, pl.ds(i * 16, 16), u * 128 : (u + 1) * 128] = tmp_a[u, 0:16, :].astype(jnp.bfloat16)
            return carry

        lax.fori_loop(0, rows // 16, some, 0)

    def block(i, carry):
        slot = lax.rem(i, NO)

        @pl.when(i >= NO)
        def _():
            ocp(i - NO, slot).wait()

        start = p0 + i * RB
        whole = (start + RB <= pend) & ((start + RB <= m0) | (start >= m0))

        @pl.when(whole)
        def _():
            at = start + jnp.where(start >= m0, off1, off0)
            gather_block(units, RB, lambda j: ord_ref[at + j], src, (tmp_a, tmp_b), ost, slot)

        @pl.when(jnp.logical_not(whole))
        def _():
            mixed(start, slot, RB)

        ocp(i, slot).start()
        return carry

    lax.fori_loop(0, nb, block, 0)

    def drain(i, carry):
        ocp(i, lax.rem(i, NO)).wait()
        return carry

    lax.fori_loop(jnp.maximum(nb - NO, 0), nb, drain, 0)
    if rest:

        @pl.when(p0 + full * RB < pend)
        def _():
            mixed(p0 + full * RB, 0, rest)
            last = pltpu.make_async_copy(ost.at[0, pl.ds(0, rest)], out.at[pl.ds(full * RB, rest)], tsem)
            last.start()
            last.wait()


def pack(units, k0, cap, order, meta, own, sibl):
    return pl.pallas_call(
        functools.partial(pack_kernel, units, k0),
        out_shape=jax.ShapeDtypeStruct((cap, units * 128), jnp.bfloat16),
        in_specs=[ANY, SMEM, ANY, ANY],
        out_specs=ANY,
        scratch_shapes=[
            pltpu.VMEM((units, 2 * N, 128), jnp.float32),
            pltpu.VMEM((NS, CH, units * 128), jnp.bfloat16),
            pltpu.VMEM((units, GRP, 128), jnp.float32),
            pltpu.VMEM((units, GRP, 128), jnp.float32),
            pltpu.VMEM((NO, RB, units * 128), jnp.bfloat16),
            pltpu.SMEM((2 * N,), jnp.int32),
            pltpu.SemaphoreType.DMA((NS,)),
            pltpu.SemaphoreType.DMA((NO,)),
            pltpu.SemaphoreType.DMA,
            pltpu.SemaphoreType.DMA,
        ],
        cost_estimate=pl.CostEstimate(flops=0, transcendentals=0, bytes_accessed=2 * N * units * 256 + 8_000_000),
        compiler_params=pltpu.CompilerParams(vmem_limit_bytes=VMEM_LIMIT),
    )(order, meta, own, sibl)


def zero_kernel(meta_ref, out, zeros, sem):
    zeros[...] = jnp.zeros_like(zeros)
    nb = (meta_ref[5] + FB - 1) // FB

    def cp(i):
        return pltpu.make_async_copy(zeros, out.at[pl.ds(pl.multiple_of(i * FB, FB), FB)], sem)

    def go(i, c):
        cp(i).start()
        return c

    def end(i, c):
        cp(i).wait()
        return c

    lax.fori_loop(nb, OUT // FB, go, 0)
    lax.fori_loop(nb, OUT // FB, end, 0)


def zero_tail(meta, width):
    return pl.pallas_call(
        zero_kernel,
        out_shape=jax.ShapeDtypeStruct((OUT, width), jnp.bfloat16),
        in_specs=[SMEM],
        out_specs=ANY,
        scratch_shapes=[pltpu.VMEM((FB, width), jnp.bfloat16), pltpu.SemaphoreType.DMA],
        name="zero",
        cost_estimate=pl.CostEstimate(flops=0, transcendentals=0, bytes_accessed=OUT * width),
        compiler_params=pltpu.CompilerParams(vmem_limit_bytes=8 * 1024 * 1024),
    )(meta)


def final_kernel(
    units, k0, cap, idx, meta_ref, own, sibl, rown, rsib, prev, out, src, stage, tmp_a, tmp_b, ost, near, idx_a, idx_b,
    lsem, osem, isem, nsem
):
    nb = (meta_ref[5] + FB - 1) // FB
    lists = (idx_a, idx_b)

    def icp(i, k):
        return pltpu.make_async_copy(near.at[pl.ds(pl.multiple_of(i * FB, FB), FB)], lists[k], isem.at[k])

    fetch = pltpu.make_async_copy(idx, near, nsem)
    fetch.start()
    src[:, ZERO_ROW : ZERO_ROW + 8, :] = jnp.zeros((units, 8, 128), jnp.float32)
    ks = first_unit(sibl, units, k0)
    parts = [(own, N, k0, 0), (sibl, N, ks, N), (rown, cap, 0, 2 * N), (rsib, cap, 0, 3 * N)]
    load_rows(units, parts, src, stage, lsem)
    fetch.wait()
    for k in (0, 1):

        @pl.when(k < nb)
        def _():
            icp(k, k).start()

    def ocp(i, slot):
        return pltpu.make_async_copy(
            ost.at[slot], out.at[pl.ds(pl.multiple_of(i * FB, FB), FB), pl.ds(k0 * 128, units * 128)], osem.at[slot]
        )

    def pair(h, carry):
        for k in (0, 1):
            i = 2 * h + k

            @pl.when(i < nb)
            def _():
                slot = lax.rem(i, FO)

                @pl.when(i >= FO)
                def _():
                    ocp(i - FO, slot).wait()

                icp(i, k).wait()
                gather_block(units, FB, lambda j: lists[k][j], src, (tmp_a, tmp_b), ost, slot)
                ocp(i, slot).start()

                @pl.when(i + 2 < nb)
                def _():
                    icp(i + 2, k).start()

        return carry

    lax.fori_loop(0, (nb + 1) // 2, pair, 0)

    def drain(i, carry):
        ocp(i, lax.rem(i, FO)).wait()
        return carry

    lax.fori_loop(jnp.maximum(nb - FO, 0), nb, drain, 0)


def final(units, k0, cap, idx, meta, own, sibl, rown, rsib, prev):
    return pl.pallas_call(
        functools.partial(final_kernel, units, k0, cap),
        out_shape=jax.ShapeDtypeStruct(prev.shape, prev.dtype),
        in_specs=[ANY, SMEM, ANY, ANY, ANY, ANY, ANY],
        out_specs=ANY,
        input_output_aliases={6: 0},
        scratch_shapes=[
            pltpu.VMEM((units, ZERO_ROW + 8, 128), jnp.float32),
            pltpu.VMEM((NS, CH, units * 128), jnp.bfloat16),
            pltpu.VMEM((units, GRP, 128), jnp.float32),
            pltpu.VMEM((units, GRP, 128), jnp.float32),
            pltpu.VMEM((FO, FB, units * 128), jnp.bfloat16),
            pltpu.VMEM((OUT,), jnp.int32),
            pltpu.SMEM((FB,), jnp.int32),
            pltpu.SMEM((FB,), jnp.int32),
            pltpu.SemaphoreType.DMA((NS,)),
            pltpu.SemaphoreType.DMA((FO,)),
            pltpu.SemaphoreType.DMA((2,)),
            pltpu.SemaphoreType.DMA,
        ],
        cost_estimate=pl.CostEstimate(flops=0, transcendentals=0, bytes_accessed=4 * N * units * 256 + 10_000_000),
        compiler_params=pltpu.CompilerParams(vmem_limit_bytes=VMEM_LIMIT),
    )(idx, meta, own, sibl, rown, rsib, prev)


SIBLING = [(0, 1), (1, 0), (2, 3), (3, 2)]
ACROSS = [(0, 2), (2, 0), (1, 3), (3, 1)]


def deliver(level, order, meta, keys, codes, sib0, own):
    cap = CAPS[level]
    width = own.shape[1]
    starts = [sum(UNITS[:i]) for i in range(len(UNITS))]
    sibl = lax.ppermute(own, "g", SIBLING)
    raws = [(own, sib0)] + [(own, sibl)] * (len(UNITS) - 1)
    packed = []
    for i, (u, k0) in enumerate(zip(UNITS, starts)):
        packed.append(pack(u, k0, cap, order, meta, *raws[i]))
        meta, _ = lax.optimization_barrier((meta, packed[-1]))
        if i == 0:
            keys, codes, _ = lax.optimization_barrier((keys, codes, packed[-1]))
            mk, mc = merge(keys, codes)
            real = lax.iota(jnp.int32, OUT) < meta[5]
            mk = lax.dynamic_slice(jnp.pad(mk.reshape(-1), (0, OUT)), (meta[7],), (OUT,))
            mc = lax.dynamic_slice(jnp.pad(mc.reshape(-1), (0, OUT)), (meta[7],), (OUT,))
            out_keys = jnp.where(real, mk, PAD_KEY)
            idx = jnp.where(real, mc, ZERO_ROW)
            meta, idx = lax.optimization_barrier((meta, idx))
        if i == 1:
            out = zero_tail(meta, width)
            meta, _ = lax.optimization_barrier((meta, out))
    for i, (u, k0, p) in enumerate(zip(UNITS, starts, packed)):
        got = lax.ppermute(p, "g", ACROSS)
        relayed = lax.ppermute(got, "g", SIBLING)
        out = final(u, k0, cap, idx, meta, *raws[i], got, relayed, out)
    return out_keys, out


def solution(mesh):
    def local_part(keys_loc, rows_loc):
        gkeys, codes, ordc, meta, sib0 = plan(keys_loc.reshape(KR, 128), rows_loc)
        out_keys, out_rows = lax.switch(
            meta[6],
            [functools.partial(deliver, i) for i in range(len(CAPS))],
            ordc.reshape(-1),
            meta,
            gkeys,
            codes,
            sib0,
            rows_loc,
        )
        return out_keys, out_rows, meta[5:6]

    row_spec = P(("batch", "g"))
    mat_spec = P(("batch", "g"), None)
    return jax.shard_map(
        local_part, mesh=mesh, in_specs=(row_spec, mat_spec), out_specs=(row_spec, mat_spec, row_spec), check_vma=False
    )
```
